32 devices in a mesh: uly: 2 (over y), blk: 16 (over z, x, core).
Axes of the slice: x: 2, y: 2, z: 4, core: 2. Of those that a mesh axis runs over, the one named last changes fastest.
Arguments:
- query_inputs: bfloat16 [4096, 2048], P(('blk', 'uly')), may hold values from -6 to 6
- key_inputs: bfloat16 [4096, 1024], P(('blk', 'uly')), may hold values from -6 to 6
- value_inputs: bfloat16 [4096, 1024], P(('blk', 'uly')), may hold values from -6 to 6
- forward_out: bfloat16 [4096, 2048], P(('blk', 'uly')), may hold values from -6 to 6
- output_gradient: bfloat16 [4096, 2048], P(('blk', 'uly')), may hold values from -4 to 4
- lse_parts: float32 [4096, 16, 2], P(('blk', 'uly')), may hold values from 3 to 247
- segment_ids: int32 [4096], P(('blk', 'uly')), may hold values from 0 to 31, never falling along the last dimension, each value on 1 to 512 neighbouring positions
Outputs:
- query_grad: bfloat16 [4096, 2048], P(('blk', 'uly'))
- key_grad: bfloat16 [4096, 1024], P(('blk', 'uly'))
- value_grad: bfloat16 [4096, 1024], P(('blk', 'uly'))
The draws below stay inside these ranges and needn't reach their ends.
Inputs may be any that keep to these rules, and one draw needn't show every extreme that they name: `segment_ids`: never falls along the sequence; every document holds 1 to 512 tokens, and some document exactly 512.
All inputs are finite; a program needn't handle non-finite values.
Results may differ from the reference program's by a relative error of at most 0.0051.
Values may be sent and summed in bfloat16 or wider, within the bound.
A program may use at most 128 MiB of HBM per device.

```python
import math
import jax
import jax.numpy as jnp
import numpy as np
from jax import lax

HEAD_SIZE = 128
QUERY_HEADS = 16
KEY_VALUE_HEADS = 8
QBLOCK = 512
SEQUENCE_TOKENS = 4096
DOCUMENT_LIMIT = 512
SEGS = 32


def draw_lse_parts(key, part):
    first_key = jax.random.fold_in(key, 0)
    shape_all = (SEQUENCE_TOKENS, QUERY_HEADS, 2)
    return jnp.clip(5.0 + 0.8 * jax.random.normal(first_key, shape_all, jnp.float32), 3.0, 7.0)


def shard_levels(key, dims, cuts, least, top_value):
    def one(dim, shards_of):
        draws = jax.random.uniform(jax.random.fold_in(jax.random.fold_in(key, 6), dim), (shards_of,), jnp.float32, least / len(cuts), top_value / len(cuts))
        return jnp.repeat(jnp.exp(draws), dims[dim] // shards_of).reshape((-1,) + (1,) * (len(dims) - dim - 1))

    loudness = one(*cuts[0])
    for cut in cuts[1:]:
        loudness = loudness * one(*cut)
    return loudness


def split_up(count, total, most, slope):
    loads = [(1 << 20) // math.isqrt(grade ** slope) + 1 for grade in range(2, count + 1)]
    rest, counts = total - most - (count - 1), [1] * (count - 1)
    while rest > 0:
        candidates = [i for i in range(count - 1) if counts[i] < most]
        pool, budget = sum([loads[i] for i in candidates]), rest
        for i in candidates:
            extra = min(most - counts[i], max(1, budget * loads[i] // pool), rest)
            counts[i] = counts[i] + extra
            rest = rest - extra
    return np.array([most] + counts)


def ragged_sizes(rng, number_of, total, bound, slope):
    if number_of == 2:
        one = jax.random.randint(rng, (), max(1, total - bound), min(bound, total - 1) + 1)
        return jnp.stack([one, total - one])
    sizes = jnp.asarray(split_up(number_of, total, bound, slope), jnp.int32)
    pairs = (number_of - 1) // 2
    donor, taker = sizes[1:1 + 2 * pairs:2], sizes[2:2 + 2 * pairs:2]
    room = jnp.minimum(donor - 1, bound - taker)
    passed = jax.random.randint(jax.random.fold_in(rng, 1), (pairs,), 0, 1 << 20) % (room + 1)
    sizes = sizes.at[1:1 + 2 * pairs:2].set(donor - passed).at[2:2 + 2 * pairs:2].set(taker + passed)
    return sizes[jax.random.permutation(jax.random.fold_in(rng, 2), number_of)]


def scatter_about(rng, extent, deviation, limit, cuts=(), kind=jnp.bfloat16):
    array = jax.random.normal(rng, extent, jnp.float32) * deviation
    if len(cuts) > 0:
        array = shard_levels(rng, extent, cuts, -0.22, 0.18) * array
    return jnp.clip(array, min=-limit, max=limit).astype(kind)


def setup_inputs(seed: int = 0) -> dict:
    keys = jax.random.split(jax.random.key(seed), 8)
    return {
        "query_inputs": scatter_about(keys[0], (SEQUENCE_TOKENS, QUERY_HEADS * HEAD_SIZE), 1.0, 6.0, ((0, 32),)),
        "key_inputs": scatter_about(keys[1], (SEQUENCE_TOKENS, KEY_VALUE_HEADS * HEAD_SIZE), 1.0, 6.0, ((0, 32),)),
        "value_inputs": scatter_about(keys[2], (SEQUENCE_TOKENS, KEY_VALUE_HEADS * HEAD_SIZE), 1.0, 6.0, ((0, 32),)),
        "forward_out": scatter_about(keys[3], (SEQUENCE_TOKENS, QUERY_HEADS * HEAD_SIZE), 0.5, 6.0, ((0, 32),)),
        "output_gradient": scatter_about(keys[4], (SEQUENCE_TOKENS, QUERY_HEADS * HEAD_SIZE), 0.25, 4.0, ((0, 32),)),
        "lse_parts": draw_lse_parts(jax.random.fold_in(keys[7], 71), 0),
        "segment_ids": jnp.searchsorted(jnp.cumsum(ragged_sizes(keys[6], SEGS, SEQUENCE_TOKENS, DOCUMENT_LIMIT, 2)), jnp.arange(SEQUENCE_TOKENS), side="right").astype(jnp.int32),
    }


def merge_parts(partials):
    highest = lax.optimization_barrier(jnp.max(partials, axis=-1))
    return highest + jnp.log(lax.optimization_barrier(jnp.sum(jnp.exp(partials - highest[..., None]), axis=-1)))

def round_trip(values_in):
    rounded = lax.optimization_barrier(values_in.astype(jnp.bfloat16))
    return rounded.astype(jnp.float32)

def reference(query_inputs, key_inputs, value_inputs, forward_out, output_gradient, lse_parts, segment_ids):
    token_count = query_inputs.shape[0]
    group_width = QUERY_HEADS // KEY_VALUE_HEADS
    score_scale = 1.0 / math.sqrt(HEAD_SIZE)
    rows_per_block = min(QBLOCK, token_count)
    lookback_span = DOCUMENT_LIMIT + rows_per_block
    logsumexp_rows = merge_parts(lse_parts)
    products = output_gradient.astype(jnp.float32) * forward_out.astype(jnp.float32)
    row_deltas = lax.optimization_barrier(jnp.sum(products.reshape(token_count, QUERY_HEADS, HEAD_SIZE), axis=-1))
    key_with_padding = jnp.pad(key_inputs, ((DOCUMENT_LIMIT, 0), (0, 0)))
    value_with_padding = jnp.pad(value_inputs, ((DOCUMENT_LIMIT, 0), (0, 0)))
    ids_padded = jnp.concatenate([jnp.full((DOCUMENT_LIMIT,), -1, jnp.int32), segment_ids.astype(jnp.int32)])

    def block_step(carried, block_index):
        key_gradient_running, value_gradient_running = carried
        leading_row = (block_index * rows_per_block).astype(jnp.int32)
        query_quad = lax.dynamic_slice_in_dim(query_inputs, leading_row, rows_per_block, 0).astype(jnp.float32).reshape(rows_per_block, KEY_VALUE_HEADS, group_width, HEAD_SIZE)
        gradient_quad = lax.dynamic_slice_in_dim(output_gradient, leading_row, rows_per_block, 0).astype(jnp.float32).reshape(rows_per_block, KEY_VALUE_HEADS, group_width, HEAD_SIZE)
        logsumexp_cube = lax.dynamic_slice_in_dim(logsumexp_rows, leading_row, rows_per_block, 0).reshape(rows_per_block, KEY_VALUE_HEADS, group_width).transpose(1, 2, 0)[..., None]
        delta_cube = lax.dynamic_slice_in_dim(row_deltas, leading_row, rows_per_block, 0).reshape(rows_per_block, KEY_VALUE_HEADS, group_width).transpose(1, 2, 0)[..., None]
        key_cube = lax.dynamic_slice_in_dim(key_with_padding, leading_row, lookback_span, 0).astype(jnp.float32).reshape(lookback_span, KEY_VALUE_HEADS, HEAD_SIZE)
        value_cube = lax.dynamic_slice_in_dim(value_with_padding, leading_row, lookback_span, 0).astype(jnp.float32).reshape(lookback_span, KEY_VALUE_HEADS, HEAD_SIZE)
        query_ids = lax.dynamic_slice_in_dim(segment_ids.astype(jnp.int32), leading_row, rows_per_block, 0)
        key_ids = lax.dynamic_slice_in_dim(ids_padded, leading_row, lookback_span, 0)
        query_pos = leading_row + DOCUMENT_LIMIT + jnp.arange(rows_per_block, dtype=jnp.int32)
        key_pos = leading_row + jnp.arange(lookback_span, dtype=jnp.int32)
        allowed = (key_pos[None, :] <= query_pos[:, None]) & (key_ids[None, :] == query_ids[:, None])
        scores = jnp.einsum('mhgd,nhd->hgmn', query_quad, key_cube) * score_scale
        weights = jnp.where(allowed, jnp.exp(scores - logsumexp_cube), 0.0)
        value_portion = jnp.einsum('hgmn,mhgd->nhd', round_trip(weights), gradient_quad)
        prob_grad = jnp.einsum('mhgd,nhd->hgmn', gradient_quad, value_cube)
        score_grad = round_trip(weights * (prob_grad - delta_cube))
        query_part = jnp.einsum('hgmn,nhd->mhgd', score_grad, key_cube) * score_scale
        key_portion = jnp.einsum('hgmn,mhgd->nhd', score_grad, query_quad) * score_scale
        key_window_rows = lax.dynamic_slice_in_dim(key_gradient_running, leading_row, lookback_span, 0) + key_portion.reshape(lookback_span, KEY_VALUE_HEADS * HEAD_SIZE)
        value_window_rows = lax.dynamic_slice_in_dim(value_gradient_running, leading_row, lookback_span, 0) + value_portion.reshape(lookback_span, KEY_VALUE_HEADS * HEAD_SIZE)
        key_gradient_running = lax.dynamic_update_slice_in_dim(key_gradient_running, key_window_rows, leading_row, 0)
        value_gradient_running = lax.dynamic_update_slice_in_dim(value_gradient_running, value_window_rows, leading_row, 0)
        return ((key_gradient_running, value_gradient_running), query_part.reshape(rows_per_block, QUERY_HEADS * HEAD_SIZE).astype(jnp.bfloat16))
    initial_running = (jnp.zeros((token_count + DOCUMENT_LIMIT, KEY_VALUE_HEADS * HEAD_SIZE), jnp.float32), jnp.zeros((token_count + DOCUMENT_LIMIT, KEY_VALUE_HEADS * HEAD_SIZE), jnp.float32))
    final_acc, query_blocks = lax.scan(block_step, initial_running, jnp.arange(token_count // rows_per_block, dtype=jnp.int32))
    query_grad = query_blocks.reshape(token_count, QUERY_HEADS * HEAD_SIZE)
    key_grad = final_acc[0][DOCUMENT_LIMIT:].astype(jnp.bfloat16)
    value_grad = final_acc[1][DOCUMENT_LIMIT:].astype(jnp.bfloat16)
    return (query_grad, key_grad, value_grad)
```

```python
import functools
import math

import jax
import jax.numpy as jnp
from jax import lax
from jax.experimental import pallas as pl
from jax.experimental.pallas import tpu as pltpu
from jax.sharding import PartitionSpec as P

HEAD_SIZE = 128
QUERY_HEADS = 16
KEY_VALUE_HEADS = 8
GROUP = QUERY_HEADS // KEY_VALUE_HEADS
TILE = 256
FAR = -1e30


def merge_parts(partials):
    highest = jnp.max(partials, axis=-1)
    return highest + jnp.log(jnp.sum(jnp.exp(partials - highest[..., None]), axis=-1))


def row_delta(grad_rows, out_rows):
    row_total = grad_rows.shape[0]
    products = grad_rows.astype(jnp.float32) * out_rows.astype(jnp.float32)
    return jnp.sum(products.reshape(row_total, -1, HEAD_SIZE), axis=-1)


def dot_nt(a, b):
    return lax.dot_general(a, b, (((1,), (1,)), ((), ())), preferred_element_type=jnp.float32)


def dot_nn(a, b):
    return lax.dot_general(a, b, (((1,), (0,)), ((), ())), preferred_element_type=jnp.float32)


def dot_tn(a, b):
    return lax.dot_general(a, b, (((0,), (0,)), ((), ())), preferred_element_type=jnp.float32)


def kernel(
    uly_count, blk_count,
    q_ref, do_ref, k_ref, v_ref, stat_ref, ids_ref,
    dq_ref, dk_ref, dv_ref,
    qb, dob, kvb, statb, idb, bias,
    dqacc, acc0, acc1, acc2, dqs, ret1, ret2, in1, in2, dkvs,
    loc_sem,
    kv_s, kv_r, qd_s, qd_r, st_s, st_r, id_s, id_r,
    h2_s, h2_r, h2i_s, h2i_r, pt_s, pt_r, pti_s, pti_r,
    r1_s, r1_r, r2_s, r2_r, oq_s, oq_r, okv_s, okv_r,
):
    U, B = uly_count, blk_count
    T = q_ref.shape[0]
    R = T * U
    KH = KEY_VALUE_HEADS // U
    D = HEAD_SIZE
    GD = GROUP * D
    scale = 1.0 / math.sqrt(D)
    u = lax.axis_index("uly")
    b = lax.axis_index("blk")
    odd = lax.rem(b, 2)
    even = odd == 0
    mate = b + 1 - 2 * odd

    def at(blk, uly):
        return {"blk": blk, "uly": uly}

    def rcopy(src, dst, ssem, rsem, dev):
        return pltpu.make_async_remote_copy(
            src_ref=src, dst_ref=dst, send_sem=ssem, recv_sem=rsem,
            device_id=dev, device_id_type=pl.DeviceIdType.MESH,
        )

    def cols(first, width):
        return pl.ds(pl.multiple_of(first, 128), width)

    def rows(place):
        return pl.ds(pl.multiple_of(place * T, T), T)

    has_up2 = b + 2 < B
    has_down2 = b >= 2
    sends_mate = jnp.logical_or(even, b >= 3)

    barrier = pltpu.get_barrier_semaphore()
    for k in range(1, U):
        pl.semaphore_signal(
            barrier, inc=1, device_id=at(b, lax.rem(u + k, U)), device_id_type=pl.DeviceIdType.MESH
        )
    pl.semaphore_signal(barrier, inc=1, device_id=at(mate, u), device_id_type=pl.DeviceIdType.MESH)

    @pl.when(has_up2)
    def _():
        pl.semaphore_signal(
            barrier, inc=1, device_id=at(b + 2, u), device_id_type=pl.DeviceIdType.MESH
        )

    @pl.when(has_down2)
    def _():
        pl.semaphore_signal(
            barrier, inc=1, device_id=at(b - 2, u), device_id_type=pl.DeviceIdType.MESH
        )

    expected = U + has_up2.astype(jnp.int32) + has_down2.astype(jnp.int32)
    pl.semaphore_wait(barrier, expected)

    mine = [
        pltpu.make_async_copy(ids_ref, idb.at[0, u], loc_sem.at[0]),
        pltpu.make_async_copy(
            k_ref.at[:, cols(u * KH * D, KH * D)], kvb.at[0, 0, rows(u), :], loc_sem.at[1]
        ),
        pltpu.make_async_copy(
            v_ref.at[:, cols(u * KH * D, KH * D)], kvb.at[0, 1, rows(u), :], loc_sem.at[2]
        ),
        pltpu.make_async_copy(stat_ref.at[u], statb.at[u], loc_sem.at[3]),
        pltpu.make_async_copy(
            q_ref.at[:, cols(u * KH * GD, KH * GD)], qb.at[rows(u), :], loc_sem.at[4]
        ),
        pltpu.make_async_copy(
            do_ref.at[:, cols(u * KH * GD, KH * GD)], dob.at[rows(u), :], loc_sem.at[5]
        ),
    ]
    for copy in mine:
        copy.start()

    def id_in(k, place, dev):
        return rcopy(ids_ref, idb.at[0, place], id_s.at[k - 1], id_r.at[k - 1], dev)

    def st_in(k, place, peer, dev):
        return rcopy(stat_ref.at[peer], statb.at[place], st_s.at[k - 1], st_r.at[k - 1], dev)

    def kv_in(k, which, j, place, peer, dev):
        ref = (k_ref, v_ref)[which]
        return rcopy(
            ref.at[:, cols((peer * KH + j) * D, D)],
            kvb.at[0, which, rows(place), cols(j * D, D)],
            kv_s.at[which, j, k - 1], kv_r.at[which, j, k - 1], dev,
        )

    def qd_in(k, which, j, place, peer, dev):
        ref, buf = ((q_ref, qb), (do_ref, dob))[which]
        return rcopy(
            ref.at[:, cols((peer * KH + j) * GD, GD)],
            buf.at[rows(place), cols(j * GD, GD)],
            qd_s.at[which, j, k - 1], qd_r.at[which, j, k - 1], dev,
        )

    peers = [(k, lax.rem(u + k, U), lax.rem(u + U - k, U)) for k in range(1, U)]
    for k, to, _ in peers:
        id_in(k, u, at(b, to)).start()
    for j in range(KH):
        for k, to, _ in peers:
            for which in range(2):
                kv_in(k, which, j, u, to, at(b, to)).start()
    for k, to, _ in peers:
        st_in(k, u, to, at(b, to)).start()
    for j in range(KH):
        for k, to, _ in peers:
            for which in range(2):
                qd_in(k, which, j, u, to, at(b, to)).start()

    def h2(j):
        return rcopy(
            kvb.at[0, :, :, cols(j * D, D)], kvb.at[2, :, :, cols(j * D, D)],
            h2_s.at[j], h2_r.at[j], at(b + 2, u),
        )

    def h2id():
        return rcopy(idb.at[0], idb.at[2], h2i_s.at[0], h2i_r.at[0], at(b + 2, u))

    def pt(j):
        return rcopy(
            kvb.at[2 * odd, :, :, cols(j * D, D)], kvb.at[1, :, :, cols(j * D, D)],
            pt_s.at[j], pt_r.at[j], at(mate, u),
        )

    def ptid():
        return rcopy(idb.at[2 * odd], idb.at[1], pti_s.at[0], pti_r.at[0], at(mate, u))

    mine[0].wait()
    for k, _, frm in peers:
        id_in(k, frm, at(b, frm)).wait_recv()

    @pl.when(has_up2)
    def _():
        h2id().start()

    @pl.when(even)
    def _():
        ptid().start()

    mine[1].wait()
    mine[2].wait()
    for j in range(KH):
        for k, _, frm in peers:
            for which in range(2):
                kv_in(k, which, j, frm, frm, at(b, frm)).wait_recv()

        @pl.when(has_up2)
        def _():
            h2(j).start()

        @pl.when(even)
        def _():
            pt(j).start()

    def make_bias(hop):
        for kp in range(U):
            key_ids = jnp.broadcast_to(idb[hop, kp, 0:1, :], (T, T)).T
            for qp in range(U):
                query_ids = idb[0, qp, 0:1, :]
                good = key_ids == query_ids
                if hop == 0:
                    kpos = lax.broadcasted_iota(jnp.int32, (T, T), 0) + kp * T
                    qpos = lax.broadcasted_iota(jnp.int32, (T, T), 1) + qp * T
                    good = jnp.logical_and(good, kpos <= qpos)
                bias[hop, kp * T:(kp + 1) * T, qp * T:(qp + 1) * T] = jnp.where(good, 0.0, FAR)

    make_bias(0)

    @pl.when(has_down2)
    def _():
        h2id().wait_recv()
        make_bias(2)

        @pl.when(odd == 1)
        def _():
            ptid().start()

    def arrive2(j):
        @pl.when(has_down2)
        def _():
            h2(j).wait_recv()

            @pl.when(odd == 1)
            def _():
                pt(j).start()

    arrive2(0)

    @pl.when(b >= 1)
    def _():
        ptid().wait_recv()
        make_bias(1)

    for copy in mine[3:]:
        copy.wait()
    for k, _, frm in peers:
        st_in(k, frm, frm, at(b, frm)).wait_recv()

    tile = min(TILE, R)
    steps = R // tile
    per = tile // T if tile >= T else 1

    def stat_row(row, qt):
        parts = [statb[qt * per + i, pl.ds(row, 1), :] for i in range(per)]
        return parts[0] if per == 1 else jnp.concatenate(parts, axis=1)

    G = KH * GROUP

    def hop_grads(hop, j, acc):
        def key_step(kt, _):
            krow = pl.ds(pl.multiple_of(kt * tile, tile), tile)
            kc = kvb[hop, 0, krow, cols(j * D, D)]
            vc = kvb[hop, 1, krow, cols(j * D, D)]

            def query_step(qt, carry):
                dk, dv = carry
                qrow = pl.ds(pl.multiple_of(qt * tile, tile), tile)
                for g in range(GROUP):
                    qc = qb[qrow, cols(j * GD + g * D, D)]
                    dc = dob[qrow, cols(j * GD + g * D, D)]
                    head = j * GROUP + g
                    lse = stat_row(head, qt)
                    delta = stat_row(G + head, qt)
                    w = jnp.exp(dot_nt(kc, qc) * scale - lse + bias[hop, krow, pl.ds(pl.multiple_of(qt * tile, tile), tile)])
                    dv = dv + dot_nn(w.astype(jnp.bfloat16), dc)
                    ds = (w * (dot_nt(vc, dc) - delta)).astype(jnp.bfloat16)
                    dk = dk + dot_nn(ds, qc)
                    part = dot_tn(ds, kc)
                    dqacc[qrow, g * D:(g + 1) * D] += part
                return dk, dv

            zero = jnp.zeros((tile, D), jnp.float32)
            if steps == 1:
                dk, dv = query_step(0, (zero, zero))
            else:
                dk, dv = lax.fori_loop(0, steps, query_step, (zero, zero))
            acc[j, 0, krow, :] = (dk * scale).astype(acc.dtype)
            acc[j, 1, krow, :] = dv.astype(acc.dtype)
            return 0

        if steps == 1:
            key_step(0, 0)
        else:
            lax.fori_loop(0, steps, key_step, 0)

    def give1(j):
        return rcopy(ret1.at[j], in1.at[j], r1_s.at[j], r1_r.at[j], at(mate, u))

    def give2(j):
        return rcopy(ret2.at[j], in2.at[j], r2_s.at[j], r2_r.at[j], at(b - 2, u))

    def oq(k, j, place, dev):
        return rcopy(
            dqs.at[j, rows(place), :], dq_ref.at[:, cols((u * KH + j) * GD, GD)],
            oq_s.at[j, k - 1], oq_r.at[j, k - 1], dev,
        )

    def okv(k, which, j, place, dev):
        ref = (dk_ref, dv_ref)[which]
        return rcopy(
            dkvs.at[j, which, rows(place), :], ref.at[:, cols((u * KH + j) * D, D)],
            okv_s.at[which, j, k - 1], okv_r.at[which, j, k - 1], dev,
        )

    def compute(j):
        for k, _, frm in peers:
            for which in range(2):
                qd_in(k, which, j, frm, frm, at(b, frm)).wait_recv()
        dqacc[...] = jnp.zeros_like(dqacc)
        hop_grads(0, j, acc0)

        @pl.when(has_down2)
        def _():
            hop_grads(2, j, acc2)

        @pl.when(b >= 1)
        def _():
            pt(j).wait_recv()
            hop_grads(1, j, ret1)
            give1(j).start()

        dqs[j] = (dqacc[...] * scale).astype(jnp.bfloat16)
        for k, to, _ in peers:
            oq(k, j, to, at(b, to)).start()
        dq_ref[:, cols((u * KH + j) * GD, GD)] = dqs[j, rows(u), :]

    def stage_a(j):
        @pl.when(jnp.logical_and(odd == 1, has_down2))
        def _():
            give1(j).wait_recv()
            ret2[j] = (acc2[j] + in1[j].astype(jnp.float32)).astype(jnp.bfloat16)

        @pl.when(jnp.logical_and(even, has_down2))
        def _():
            ret2[j] = acc2[j].astype(jnp.bfloat16)

        @pl.when(has_down2)
        def _():
            give2(j).start()

    def stage_b(j):
        @pl.when(even)
        def _():
            give1(j).wait_recv()
            acc0[j] += in1[j].astype(jnp.float32)

        @pl.when(has_up2)
        def _():
            give2(j).wait_recv()
            acc0[j] += in2[j].astype(jnp.float32)

        dkvs[j] = acc0[j].astype(jnp.bfloat16)
        for k, to, _ in peers:
            for which in range(2):
                okv(k, which, j, to, at(b, to)).start()
        for which in range(2):
            ref = (dk_ref, dv_ref)[which]
            ref[:, cols((u * KH + j) * D, D)] = dkvs[j, which, rows(u), :]

    def head_step(j, _):
        @pl.when(j + 1 < KH)
        def _():
            arrive2(jnp.minimum(j + 1, KH - 1))

        compute(j)

        @pl.when(j >= 1)
        def _():
            stage_a(jnp.maximum(j - 1, 0))

        @pl.when(j >= 2)
        def _():
            stage_b(jnp.maximum(j - 2, 0))

        return 0

    lax.fori_loop(0, KH, head_step, 0)
    stage_a(KH - 1)
    if KH >= 2:
        stage_b(KH - 2)
    stage_b(KH - 1)

    for k, to, frm in peers:
        id_in(k, u, at(b, to)).wait_send()
        st_in(k, u, to, at(b, to)).wait_send()

    @pl.when(has_up2)
    def _():
        h2id().wait_send()

    @pl.when(sends_mate)
    def _():
        ptid().wait_send()

    def finish(j, _):
        for k, to, frm in peers:
            for which in range(2):
                kv_in(k, which, j, u, to, at(b, to)).wait_send()
                qd_in(k, which, j, u, to, at(b, to)).wait_send()

        @pl.when(has_up2)
        def _():
            h2(j).wait_send()

        @pl.when(sends_mate)
        def _():
            pt(j).wait_send()

        @pl.when(b >= 1)
        def _():
            give1(j).wait_send()

        @pl.when(has_down2)
        def _():
            give2(j).wait_send()

        for k, to, frm in peers:
            oq(k, j, to, at(b, to)).wait_send()
            for which in range(2):
                okv(k, which, j, to, at(b, to)).wait_send()
            rcopy(
                dqs.at[j, rows(frm), :], dq_ref.at[:, cols((frm * KH + j) * GD, GD)],
                oq_s.at[j, k - 1], oq_r.at[j, k - 1], at(b, frm),
            ).wait_recv()
            for which in range(2):
                ref = (dk_ref, dv_ref)[which]
                rcopy(
                    dkvs.at[j, which, rows(frm), :], ref.at[:, cols((frm * KH + j) * D, D)],
                    okv_s.at[which, j, k - 1], okv_r.at[which, j, k - 1], at(b, frm),
                ).wait_recv()
        return 0

    lax.fori_loop(0, KH, finish, 0)


def per_device(uly_count, blk_count, q, k, v, out, grad, lse_parts, segment_ids):
    U, B = uly_count, blk_count
    T = q.shape[0]
    R = T * U
    KH = KEY_VALUE_HEADS // U
    G = KH * GROUP
    D = HEAD_SIZE
    lse = merge_parts(lse_parts).T.reshape(U, G, T)
    delta = row_delta(grad, out).T.reshape(U, G, T)
    stat_rows = -(-2 * G // 8) * 8
    stat = jnp.concatenate([lse, delta], axis=1)
    stat = jnp.pad(stat, ((0, 0), (0, stat_rows - 2 * G), (0, 0)))
    ids = jnp.broadcast_to(segment_ids.astype(jnp.float32)[None, :], (8, T))
    bf, f32 = jnp.bfloat16, jnp.float32
    n = max(U - 1, 1)
    dma = pltpu.SemaphoreType.DMA
    sems = []
    for shape in [(2, KH, n), (2, KH, n), (n,), (n,), (KH,), (1,), (KH,), (1,), (KH,), (KH,), (KH, n), (2, KH, n)]:
        sems += [dma(shape), dma(shape)]
    vm = pltpu.VMEM
    return pl.pallas_call(
        functools.partial(kernel, U, B),
        out_shape=(
            jax.ShapeDtypeStruct(q.shape, bf),
            jax.ShapeDtypeStruct(k.shape, bf),
            jax.ShapeDtypeStruct(v.shape, bf),
        ),
        in_specs=[pl.BlockSpec(memory_space=vm)] * 6,
        out_specs=tuple([pl.BlockSpec(memory_space=vm)] * 3),
        scratch_shapes=[
            vm((R, G * D), bf),
            vm((R, G * D), bf),
            vm((3, 2, R, KH * D), bf),
            vm((U, stat_rows, T), f32),
            vm((3, U, 8, T), f32),
            vm((3, R, R), f32),
            vm((R, GROUP * D), f32),
            vm((KH, 2, R, D), f32),
            vm((8, 128), f32),
            vm((KH, 2, R, D), f32),
            vm((KH, R, GROUP * D), bf),
            vm((KH, 2, R, D), bf),
            vm((KH, 2, R, D), bf),
            vm((KH, 2, R, D), bf),
            vm((KH, 2, R, D), bf),
            vm((KH, 2, R, D), bf),
            dma((6,)),
        ] + sems,
        compiler_params=pltpu.CompilerParams(
            collective_id=0, has_side_effects=True, vmem_limit_bytes=56 * 1024 * 1024
        ),
    )(q, grad, k, v, stat, ids)


def solution(mesh):
    spec = P(("blk", "uly"), None)
    body = functools.partial(per_device, mesh.shape["uly"], mesh.shape["blk"])
    return jax.shard_map(
        body,
        mesh=mesh,
        in_specs=(spec, spec, spec, spec, spec, P(("blk", "uly"), None, None), P(("blk", "uly"))),
        out_specs=(spec, spec, spec),
        check_vma=False,
    )
```

```python
import functools
import math

import jax
import jax.numpy as jnp
from jax import lax
from jax.experimental import pallas as pl
from jax.experimental.pallas import tpu as pltpu
from jax.sharding import PartitionSpec as P

HEAD_SIZE = 128
QUERY_HEADS = 16
KEY_VALUE_HEADS = 8
GROUP = QUERY_HEADS // KEY_VALUE_HEADS
TILE = 256
FAR = -1e30


def dot_nt(a, b):
    return lax.dot_general(a, b, (((1,), (1,)), ((), ())), preferred_element_type=jnp.float32)


def dot_nn(a, b):
    return lax.dot_general(a, b, (((1,), (0,)), ((), ())), preferred_element_type=jnp.float32)


def dot_tn(a, b):
    return lax.dot_general(a, b, (((0,), (0,)), ((), ())), preferred_element_type=jnp.float32)


def kernel(
    uly_count, blk_count,
    q_ref, do_hbm, k_hbm, v_hbm, out_hbm, lp_hbm, ids_hbm,
    dq_ref, dk_ref, dv_ref,
    qb, dob, kvb, statb, idb, bias,
    dqacc, acc0, acc2, dqs, ret1, ret2, in1, in2, dkvs,
    do_ref, k_ref, v_ref, out_ref, lp_ref, ids_ref, stat_ref,
    loc_sem,
    kv_s, kv_r, qd_s, qd_r, st_s, st_r, id_s, id_r,
    h2_s, h2_r, h2i_s, h2i_r, pt_s, pt_r, pti_s, pti_r,
    r1_s, r1_r, r2_s, r2_r, oq_s, oq_r, okv_s, okv_r,
):
    U, B = uly_count, blk_count
    T = q_ref.shape[0]
    R = T * U
    KH = KEY_VALUE_HEADS // U
    D = HEAD_SIZE
    GD = GROUP * D
    scale = 1.0 / math.sqrt(D)
    u = lax.axis_index("uly")
    b = lax.axis_index("blk")
    odd = lax.rem(b, 2)
    even = odd == 0
    mate = b + 1 - 2 * odd

    def at(blk, uly):
        return {"blk": blk, "uly": uly}

    def rcopy(src, dst, ssem, rsem, dev):
        return pltpu.make_async_remote_copy(
            src_ref=src, dst_ref=dst, send_sem=ssem, recv_sem=rsem,
            device_id=dev, device_id_type=pl.DeviceIdType.MESH,
        )

    def cols(first, width):
        return pl.ds(pl.multiple_of(first, 128), width)

    def rows(place):
        return pl.ds(pl.multiple_of(place * T, T), T)

    has_up2 = b + 2 < B
    has_down2 = b >= 2
    sends_mate = jnp.logical_or(even, b >= 3)

    loads = [
        pltpu.make_async_copy(src, dst, loc_sem.at[5 + i])
        for i, (src, dst) in enumerate([
            (ids_hbm, ids_ref), (k_hbm, k_ref), (v_hbm, v_ref),
            (do_hbm, do_ref), (out_hbm, out_ref), (lp_hbm, lp_ref),
        ])
    ]
    for copy in loads:
        copy.start()

    barrier = pltpu.get_barrier_semaphore()
    for k in range(1, U):
        pl.semaphore_signal(
            barrier, inc=1, device_id=at(b, lax.rem(u + k, U)), device_id_type=pl.DeviceIdType.MESH
        )
    pl.semaphore_signal(barrier, inc=1, device_id=at(mate, u), device_id_type=pl.DeviceIdType.MESH)

    @pl.when(has_up2)
    def _():
        pl.semaphore_signal(
            barrier, inc=1, device_id=at(b + 2, u), device_id_type=pl.DeviceIdType.MESH
        )

    @pl.when(has_down2)
    def _():
        pl.semaphore_signal(
            barrier, inc=1, device_id=at(b - 2, u), device_id_type=pl.DeviceIdType.MESH
        )

    expected = U + has_up2.astype(jnp.int32) + has_down2.astype(jnp.int32)
    pl.semaphore_wait(barrier, expected)

    own_q = [
        pltpu.make_async_copy(
            q_ref.at[:, cols(u * KH * GD, KH * GD)], qb.at[rows(u), :], loc_sem.at[0]
        ),
        pltpu.make_async_copy(
            do_hbm.at[:, cols(u * KH * GD, KH * GD)], dob.at[rows(u), :], loc_sem.at[1]
        ),
    ]
    own_kv = [
        pltpu.make_async_copy(
            k_hbm.at[:, cols(u * KH * D, KH * D)], kvb.at[0, 0, rows(u), :], loc_sem.at[2]
        ),
        pltpu.make_async_copy(
            v_hbm.at[:, cols(u * KH * D, KH * D)], kvb.at[0, 1, rows(u), :], loc_sem.at[3]
        ),
    ]
    own_id = pltpu.make_async_copy(ids_hbm, idb.at[0, u], loc_sem.at[4])

    def id_in(k, place, dev):
        return rcopy(ids_ref, idb.at[0, place], id_s.at[k - 1], id_r.at[k - 1], dev)

    def st_in(k, place, peer, dev):
        return rcopy(stat_ref.at[peer], statb.at[place], st_s.at[k - 1], st_r.at[k - 1], dev)

    def kv_in(k, which, j, place, peer, dev):
        ref = (k_ref, v_ref)[which]
        return rcopy(
            ref.at[:, cols((peer * KH + j) * D, D)],
            kvb.at[0, which, rows(place), cols(j * D, D)],
            kv_s.at[which, j, k - 1], kv_r.at[which, j, k - 1], dev,
        )

    def qd_in(k, which, j, place, peer, dev):
        ref, buf = ((q_ref, qb), (do_ref, dob))[which]
        return rcopy(
            ref.at[:, cols((peer * KH + j) * GD, GD)],
            buf.at[rows(place), cols(j * GD, GD)],
            qd_s.at[which, j, k - 1], qd_r.at[which, j, k - 1], dev,
        )

    peers = [(k, lax.rem(u + k, U), lax.rem(u + U - k, U)) for k in range(1, U)]
    loads[0].wait()
    for k, to, _ in peers:
        id_in(k, u, at(b, to)).start()
    loads[1].wait()
    loads[2].wait()
    for j in range(KH):
        for k, to, _ in peers:
            for which in range(2):
                kv_in(k, which, j, u, to, at(b, to)).start()
    for copy in [own_id] + own_kv + own_q:
        copy.start()

    for copy in loads[3:]:
        copy.wait()
    G = KH * GROUP
    lane = lax.broadcasted_iota(jnp.int32, (T, 128), 1)
    table = jnp.zeros((T, 128), jnp.float32)
    for h in range(U * G):
        piece = slice(h * D, (h + 1) * D)
        total = jnp.sum(
            do_ref[:, piece].astype(jnp.float32) * out_ref[:, piece].astype(jnp.float32),
            axis=1, keepdims=True,
        )
        table = jnp.where(lane == h, total, table)
    table = table.T
    part0, part1 = lp_ref[:, 0, :], lp_ref[:, 1, :]
    highest = jnp.maximum(part0, part1)
    lse_rows = highest + jnp.log(jnp.exp(part0 - highest) + jnp.exp(part1 - highest))
    for p in range(U):
        stat_ref[p, :G, :] = lse_rows[p * G:(p + 1) * G]
        stat_ref[p, G:2 * G, :] = table[p * G:(p + 1) * G]
    statb[u] = stat_ref[u]

    for j in range(KH):
        for k, to, _ in peers:
            for which in range(2):
                qd_in(k, which, j, u, to, at(b, to)).start()
        if j == 0:
            for k, to, _ in peers:
                st_in(k, u, to, at(b, to)).start()

    def h2(j):
        return rcopy(
            kvb.at[0, :, :, cols(j * D, D)], kvb.at[2, :, :, cols(j * D, D)],
            h2_s.at[j], h2_r.at[j], at(b + 2, u),
        )

    def h2id():
        return rcopy(idb.at[0], idb.at[2], h2i_s.at[0], h2i_r.at[0], at(b + 2, u))

    def pt(j):
        return rcopy(
            kvb.at[2 * odd, :, :, cols(j * D, D)], kvb.at[1, :, :, cols(j * D, D)],
            pt_s.at[j], pt_r.at[j], at(mate, u),
        )

    def ptid():
        return rcopy(idb.at[2 * odd], idb.at[1], pti_s.at[0], pti_r.at[0], at(mate, u))

    own_id.wait()
    for k, _, frm in peers:
        id_in(k, frm, at(b, frm)).wait_recv()

    @pl.when(has_up2)
    def _():
        h2id().start()

    @pl.when(even)
    def _():
        ptid().start()

    for copy in own_kv:
        copy.wait()
    for j in range(KH):
        for k, _, frm in peers:
            for which in range(2):
                kv_in(k, which, j, frm, frm, at(b, frm)).wait_recv()

        @pl.when(has_up2)
        def _():
            h2(j).start()

        @pl.when(even)
        def _():
            pt(j).start()

    def make_bias(hop):
        for kp in range(U):
            key_ids = jnp.broadcast_to(idb[hop, kp, 0:1, :].astype(jnp.float32), (T, T)).T
            for qp in range(U):
                query_ids = idb[0, qp, 0:1, :].astype(jnp.float32)
                good = key_ids == query_ids
                if hop == 0:
                    kpos = lax.broadcasted_iota(jnp.int32, (T, T), 0) + kp * T
                    qpos = lax.broadcasted_iota(jnp.int32, (T, T), 1) + qp * T
                    good = jnp.logical_and(good, kpos <= qpos)
                bias[hop, kp * T:(kp + 1) * T, qp * T:(qp + 1) * T] = jnp.where(good, 0.0, FAR)

    make_bias(0)

    @pl.when(has_down2)
    def _():
        h2id().wait_recv()
        make_bias(2)

        @pl.when(odd == 1)
        def _():
            ptid().start()

    def arrive2(j):
        @pl.when(has_down2)
        def _():
            h2(j).wait_recv()

            @pl.when(odd == 1)
            def _():
                pt(j).start()

    arrive2(0)

    @pl.when(b >= 1)
    def _():
        ptid().wait_recv()
        make_bias(1)

    for copy in own_q:
        copy.wait()
    for k, _, frm in peers:
        st_in(k, frm, frm, at(b, frm)).wait_recv()

    tile = min(TILE, R)
    steps = R // tile
    per = tile // T if tile >= T else 1

    def stat_row(row, qt):
        parts = [statb[qt * per + i, pl.ds(row, 1), :] for i in range(per)]
        return parts[0] if per == 1 else jnp.concatenate(parts, axis=1)

    def hop_grads(hop, j, acc):
        def key_step(kt, _):
            krow = pl.ds(pl.multiple_of(kt * tile, tile), tile)
            kc = kvb[hop, 0, krow, cols(j * D, D)]
            vc = kvb[hop, 1, krow, cols(j * D, D)]

            def query_step(qt, carry):
                dk, dv = carry
                qrow = pl.ds(pl.multiple_of(qt * tile, tile), tile)
                for g in range(GROUP):
                    qc = qb[qrow, cols(j * GD + g * D, D)]
                    dc = dob[qrow, cols(j * GD + g * D, D)]
                    head = j * GROUP + g
                    lse = stat_row(head, qt)
                    delta = stat_row(G + head, qt)
                    w = jnp.exp(dot_nt(kc, qc) * scale - lse + bias[hop, krow, pl.ds(pl.multiple_of(qt * tile, tile), tile)])
                    dv = dv + dot_nn(w.astype(jnp.bfloat16), dc)
                    ds = (w * (dot_nt(vc, dc) - delta)).astype(jnp.bfloat16)
                    dk = dk + dot_nn(ds, qc)
                    part = dot_tn(ds, kc)
                    dqacc[qrow, g * D:(g + 1) * D] += part
                return dk, dv

            zero = jnp.zeros((tile, D), jnp.float32)
            if steps == 1:
                dk, dv = query_step(0, (zero, zero))
            else:
                dk, dv = lax.fori_loop(0, steps, query_step, (zero, zero))
            acc[j, 0, krow, :] = (dk * scale).astype(acc.dtype)
            acc[j, 1, krow, :] = dv.astype(acc.dtype)
            return 0

        if steps == 1:
            key_step(0, 0)
        else:
            lax.fori_loop(0, steps, key_step, 0)

    def give1(j):
        return rcopy(ret1.at[j], in1.at[j], r1_s.at[j], r1_r.at[j], at(mate, u))

    def give2(j):
        return rcopy(ret2.at[j], in2.at[j], r2_s.at[j], r2_r.at[j], at(b - 2, u))

    def oq(k, j, place, dev):
        return rcopy(
            dqs.at[j, rows(place), :], dq_ref.at[:, cols((u * KH + j) * GD, GD)],
            oq_s.at[j, k - 1], oq_r.at[j, k - 1], dev,
        )

    def okv(k, which, j, place, dev):
        ref = (dk_ref, dv_ref)[which]
        return rcopy(
            dkvs.at[j, which, rows(place), :], ref.at[:, cols((u * KH + j) * D, D)],
            okv_s.at[which, j, k - 1], okv_r.at[which, j, k - 1], dev,
        )

    def compute(j):
        for k, _, frm in peers:
            for which in range(2):
                qd_in(k, which, j, frm, frm, at(b, frm)).wait_recv()
        dqacc[...] = jnp.zeros_like(dqacc)

        @pl.when(b >= 1)
        def _():
            pt(j).wait_recv()
            hop_grads(1, j, ret1)
            give1(j).start()

        @pl.when(has_down2)
        def _():
            hop_grads(2, j, acc2)

        stage_a(j)
        hop_grads(0, j, acc0)

        dqs[j] = (dqacc[...] * scale).astype(jnp.bfloat16)
        for k, to, _ in peers:
            oq(k, j, to, at(b, to)).start()
        dq_ref[:, cols((u * KH + j) * GD, GD)] = dqs[j, rows(u), :]

    def stage_a(j):
        @pl.when(jnp.logical_and(odd == 1, has_down2))
        def _():
            give1(j).wait_recv()
            ret2[j] = (acc2[j] + in1[j].astype(jnp.float32)).astype(jnp.bfloat16)

        @pl.when(jnp.logical_and(even, has_down2))
        def _():
            ret2[j] = acc2[j].astype(jnp.bfloat16)

        @pl.when(has_down2)
        def _():
            give2(j).start()

    def stage_b(j):
        @pl.when(even)
        def _():
            give1(j).wait_recv()
            acc0[j] += in1[j].astype(jnp.float32)

        @pl.when(has_up2)
        def _():
            give2(j).wait_recv()
            acc0[j] += in2[j].astype(jnp.float32)

        dkvs[j] = acc0[j].astype(jnp.bfloat16)
        for k, to, _ in peers:
            for which in range(2):
                okv(k, which, j, to, at(b, to)).start()
        for which in range(2):
            ref = (dk_ref, dv_ref)[which]
            ref[:, cols((u * KH + j) * D, D)] = dkvs[j, which, rows(u), :]

    def head_step(j, _):
        @pl.when(j + 1 < KH)
        def _():
            arrive2(jnp.minimum(j + 1, KH - 1))

        compute(j)

        @pl.when(j >= 2)
        def _():
            stage_b(jnp.maximum(j - 2, 0))

        return 0

    lax.fori_loop(0, KH, head_step, 0)
    if KH >= 2:
        stage_b(KH - 2)
    stage_b(KH - 1)

    for k, to, frm in peers:
        id_in(k, u, at(b, to)).wait_send()
        st_in(k, u, to, at(b, to)).wait_send()

    @pl.when(has_up2)
    def _():
        h2id().wait_send()

    @pl.when(sends_mate)
    def _():
        ptid().wait_send()

    def finish(j, _):
        for k, to, frm in peers:
            for which in range(2):
                kv_in(k, which, j, u, to, at(b, to)).wait_send()
                qd_in(k, which, j, u, to, at(b, to)).wait_send()

        @pl.when(has_up2)
        def _():
            h2(j).wait_send()

        @pl.when(sends_mate)
        def _():
            pt(j).wait_send()

        @pl.when(b >= 1)
        def _():
            give1(j).wait_send()

        @pl.when(has_down2)
        def _():
            give2(j).wait_send()

        for k, to, frm in peers:
            oq(k, j, to, at(b, to)).wait_send()
            for which in range(2):
                okv(k, which, j, to, at(b, to)).wait_send()
            rcopy(
                dqs.at[j, rows(frm), :], dq_ref.at[:, cols((frm * KH + j) * GD, GD)],
                oq_s.at[j, k - 1], oq_r.at[j, k - 1], at(b, frm),
            ).wait_recv()
            for which in range(2):
                ref = (dk_ref, dv_ref)[which]
                rcopy(
                    dkvs.at[j, which, rows(frm), :], ref.at[:, cols((frm * KH + j) * D, D)],
                    okv_s.at[which, j, k - 1], okv_r.at[which, j, k - 1], at(b, frm),
                ).wait_recv()
        return 0

    lax.fori_loop(0, KH, finish, 0)


def per_device(uly_count, blk_count, q, k, v, out, grad, lse_parts, segment_ids):
    U, B = uly_count, blk_count
    T = q.shape[0]
    R = T * U
    KH = KEY_VALUE_HEADS // U
    G = KH * GROUP
    D = HEAD_SIZE
    stat_rows = -(-2 * G // 8) * 8
    parts = lse_parts.transpose(1, 2, 0)
    ids = segment_ids.reshape(1, T)
    bf, f32 = jnp.bfloat16, jnp.float32
    n = max(U - 1, 1)
    dma = pltpu.SemaphoreType.DMA
    sems = []
    for shape in [(2, KH, n), (2, KH, n), (n,), (n,), (KH,), (1,), (KH,), (1,), (KH,), (KH,), (KH, n), (2, KH, n)]:
        sems += [dma(shape), dma(shape)]
    vm = pltpu.VMEM
    return pl.pallas_call(
        functools.partial(kernel, U, B),
        out_shape=(
            jax.ShapeDtypeStruct(q.shape, bf),
            jax.ShapeDtypeStruct(k.shape, bf),
            jax.ShapeDtypeStruct(v.shape, bf),
        ),
        in_specs=[pl.BlockSpec(memory_space=pltpu.HBM)] * 7,
        out_specs=tuple([pl.BlockSpec(memory_space=vm)] * 3),
        scratch_shapes=[
            vm((R, G * D), bf),
            vm((R, G * D), bf),
            vm((3, 2, R, KH * D), bf),
            vm((U, stat_rows, T), f32),
            vm((3, U, 1, T), jnp.int32),
            vm((3, R, R), f32),
            vm((R, GROUP * D), f32),
            vm((KH, 2, R, D), f32),
            vm((KH, 2, R, D), f32),
            vm((KH, R, GROUP * D), bf),
            vm((KH, 2, R, D), bf),
            vm((KH, 2, R, D), bf),
            vm((KH, 2, R, D), bf),
            vm((KH, 2, R, D), bf),
            vm((KH, 2, R, D), bf),
            vm(q.shape, bf),
            vm(k.shape, bf),
            vm(v.shape, bf),
            vm(q.shape, bf),
            vm(parts.shape, f32),
            vm((1, T), jnp.int32),
            vm((U, stat_rows, T), f32),
            dma((11,)),
        ] + sems,
        compiler_params=pltpu.CompilerParams(
            collective_id=0, has_side_effects=True, vmem_limit_bytes=56 << 20
        ),
    )(q, grad, k, v, out, parts, ids)


def solution(mesh):
    spec = P(("blk", "uly"), None)
    body = functools.partial(per_device, mesh.shape["uly"], mesh.shape["blk"])
    return jax.shard_map(
        body,
        mesh=mesh,
        in_specs=(spec, spec, spec, spec, spec, P(("blk", "uly"), None, None), P(("blk", "uly"))),
        out_specs=(spec, spec, spec),
        check_vma=False,
    )
```

```python
import functools
import math

import jax
import jax.numpy as jnp
from jax import lax
from jax.experimental import pallas as pl
from jax.experimental.pallas import tpu as pltpu
from jax.sharding import PartitionSpec as P

HEAD_SIZE = 128
QUERY_HEADS = 16
KEY_VALUE_HEADS = 8
GROUP = QUERY_HEADS // KEY_VALUE_HEADS
TILE = 256
PIECES = 2
FAR = -1e30


def dot_nt(a, b):
    return lax.dot_general(a, b, (((1,), (1,)), ((), ())), preferred_element_type=jnp.float32)


def dot_nn(a, b):
    return lax.dot_general(a, b, (((1,), (0,)), ((), ())), preferred_element_type=jnp.float32)


def dot_tn(a, b):
    return lax.dot_general(a, b, (((0,), (0,)), ((), ())), preferred_element_type=jnp.float32)


def kernel(
    uly_count, blk_count,
    q_ref, do_hbm, k_hbm, v_hbm, out_hbm, lp_hbm, ids_hbm,
    dq_ref, dk_ref, dv_ref,
    qb, dob, kvb, statb, idb, bias,
    dqacc, acc0, acc2, dqs, ret1, ret2, in1, in2, dkvs,
    do_ref, k_ref, v_ref, out_ref, lp_ref, ids_ref, stat_ref,
    loc_sem, keep_sem,
    kv_s, kv_r, qd_s, qd_r, st_s, st_r, id_s, id_r,
    h2_s, h2_r, h2i_s, h2i_r, pt_s, pt_r, pti_s, pti_r,
    r1_s, r1_r, r2_s, r2_r, oq_s, oq_r, okv_s, okv_r,
):
    U, B = uly_count, blk_count
    T = q_ref.shape[0]
    R = T * U
    KH = KEY_VALUE_HEADS // U
    D = HEAD_SIZE
    GD = GROUP * D
    scale = 1.0 / math.sqrt(D)
    u = lax.axis_index("uly")
    b = lax.axis_index("blk")
    odd = lax.rem(b, 2)
    even = odd == 0
    mate = b + 1 - 2 * odd

    def at(blk, uly):
        return {"blk": blk, "uly": uly}

    def rcopy(src, dst, ssem, rsem, dev):
        return pltpu.make_async_remote_copy(
            src_ref=src, dst_ref=dst, send_sem=ssem, recv_sem=rsem,
            device_id=dev, device_id_type=pl.DeviceIdType.MESH,
        )

    def cols(first, width):
        return pl.ds(pl.multiple_of(first, 128), width)

    def rows(place):
        return pl.ds(pl.multiple_of(place * T, T), T)

    has_up2 = b + 2 < B
    has_down2 = b >= 2
    sends_mate = jnp.logical_or(even, b >= 3)

    loads = [
        pltpu.make_async_copy(src, dst, loc_sem.at[5 + i])
        for i, (src, dst) in enumerate([
            (ids_hbm, ids_ref), (k_hbm, k_ref), (v_hbm, v_ref),
            (do_hbm, do_ref), (out_hbm, out_ref), (lp_hbm, lp_ref),
        ])
    ]
    for copy in loads:
        copy.start()

    barrier = pltpu.get_barrier_semaphore()
    for k in range(1, U):
        pl.semaphore_signal(
            barrier, inc=1, device_id=at(b, lax.rem(u + k, U)), device_id_type=pl.DeviceIdType.MESH
        )
    pl.semaphore_signal(barrier, inc=1, device_id=at(mate, u), device_id_type=pl.DeviceIdType.MESH)

    @pl.when(has_up2)
    def _():
        pl.semaphore_signal(
            barrier, inc=1, device_id=at(b + 2, u), device_id_type=pl.DeviceIdType.MESH
        )

    @pl.when(has_down2)
    def _():
        pl.semaphore_signal(
            barrier, inc=1, device_id=at(b - 2, u), device_id_type=pl.DeviceIdType.MESH
        )

    expected = U + has_up2.astype(jnp.int32) + has_down2.astype(jnp.int32)
    pl.semaphore_wait(barrier, expected)

    own_q = [
        pltpu.make_async_copy(
            q_ref.at[:, cols(u * KH * GD, KH * GD)], qb.at[rows(u), :], loc_sem.at[0]
        ),
        pltpu.make_async_copy(
            do_hbm.at[:, cols(u * KH * GD, KH * GD)], dob.at[rows(u), :], loc_sem.at[1]
        ),
    ]
    own_kv = [
        pltpu.make_async_copy(
            k_hbm.at[:, cols(u * KH * D, KH * D)], kvb.at[0, 0, rows(u), :], loc_sem.at[2]
        ),
        pltpu.make_async_copy(
            v_hbm.at[:, cols(u * KH * D, KH * D)], kvb.at[0, 1, rows(u), :], loc_sem.at[3]
        ),
    ]
    own_id = pltpu.make_async_copy(ids_hbm, idb.at[0, u], loc_sem.at[4])

    def id_in(k, place, dev):
        return rcopy(ids_ref, idb.at[0, place], id_s.at[k - 1], id_r.at[k - 1], dev)

    def st_in(k, place, peer, dev):
        return rcopy(stat_ref.at[peer], statb.at[place], st_s.at[k - 1], st_r.at[k - 1], dev)

    def kv_in(k, which, j, place, peer, dev):
        ref = (k_ref, v_ref)[which]
        return rcopy(
            ref.at[:, cols((peer * KH + j) * D, D)],
            kvb.at[0, which, rows(place), cols(j * D, D)],
            kv_s.at[which, j, k - 1], kv_r.at[which, j, k - 1], dev,
        )

    def qd_in(k, which, j, place, peer, dev):
        ref, buf = ((q_ref, qb), (do_ref, dob))[which]
        return rcopy(
            ref.at[:, cols((peer * KH + j) * GD, GD)],
            buf.at[rows(place), cols(j * GD, GD)],
            qd_s.at[which, j, k - 1], qd_r.at[which, j, k - 1], dev,
        )

    peers = [(k, lax.rem(u + k, U), lax.rem(u + U - k, U)) for k in range(1, U)]
    loads[0].wait()
    for k, to, _ in peers:
        id_in(k, u, at(b, to)).start()
    loads[1].wait()
    loads[2].wait()
    for j in range(KH):
        for k, to, _ in peers:
            for which in range(2):
                kv_in(k, which, j, u, to, at(b, to)).start()
    for copy in [own_id] + own_kv + own_q:
        copy.start()

    for copy in loads[3:]:
        copy.wait()
    G = KH * GROUP
    lane = lax.broadcasted_iota(jnp.int32, (T, 128), 1)
    table = jnp.zeros((T, 128), jnp.float32)
    for h in range(U * G):
        piece = slice(h * D, (h + 1) * D)
        total = jnp.sum(
            do_ref[:, piece].astype(jnp.float32) * out_ref[:, piece].astype(jnp.float32),
            axis=1, keepdims=True,
        )
        table = jnp.where(lane == h, total, table)
    table = table.T
    part0, part1 = lp_ref[:, 0, :], lp_ref[:, 1, :]
    highest = jnp.maximum(part0, part1)
    lse_rows = highest + jnp.log(jnp.exp(part0 - highest) + jnp.exp(part1 - highest))
    for p in range(U):
        stat_ref[p, :G, :] = lse_rows[p * G:(p + 1) * G]
        stat_ref[p, G:2 * G, :] = table[p * G:(p + 1) * G]
    statb[u] = stat_ref[u]

    for j in range(KH):
        for k, to, _ in peers:
            for which in range(2):
                qd_in(k, which, j, u, to, at(b, to)).start()
        if j == 0:
            for k, to, _ in peers:
                st_in(k, u, to, at(b, to)).start()

    def h2(j):
        return rcopy(
            kvb.at[0, :, :, cols(j * D, D)], kvb.at[2, :, :, cols(j * D, D)],
            h2_s.at[j], h2_r.at[j], at(b + 2, u),
        )

    def h2id():
        return rcopy(idb.at[0], idb.at[2], h2i_s.at[0], h2i_r.at[0], at(b + 2, u))

    def pt(j):
        return rcopy(
            kvb.at[2 * odd, :, :, cols(j * D, D)], kvb.at[1, :, :, cols(j * D, D)],
            pt_s.at[j], pt_r.at[j], at(mate, u),
        )

    def ptid():
        return rcopy(idb.at[2 * odd], idb.at[1], pti_s.at[0], pti_r.at[0], at(mate, u))

    own_id.wait()
    for k, _, frm in peers:
        id_in(k, frm, at(b, frm)).wait_recv()

    @pl.when(has_up2)
    def _():
        h2id().start()

    @pl.when(even)
    def _():
        ptid().start()

    for copy in own_kv:
        copy.wait()
    for j in range(KH):
        for k, _, frm in peers:
            for which in range(2):
                kv_in(k, which, j, frm, frm, at(b, frm)).wait_recv()

        @pl.when(has_up2)
        def _():
            h2(j).start()

        @pl.when(even)
        def _():
            pt(j).start()

    def make_bias(hop):
        for kp in range(U):
            key_ids = jnp.broadcast_to(idb[hop, kp, 0:1, :].astype(jnp.float32), (T, T)).T
            for qp in range(U):
                query_ids = idb[0, qp, 0:1, :].astype(jnp.float32)
                good = key_ids == query_ids
                if hop == 0:
                    kpos = lax.broadcasted_iota(jnp.int32, (T, T), 0) + kp * T
                    qpos = lax.broadcasted_iota(jnp.int32, (T, T), 1) + qp * T
                    good = jnp.logical_and(good, kpos <= qpos)
                bias[hop, kp * T:(kp + 1) * T, qp * T:(qp + 1) * T] = jnp.where(good, 0.0, FAR)

    make_bias(0)

    @pl.when(has_down2)
    def _():
        h2id().wait_recv()
        make_bias(2)

        @pl.when(odd == 1)
        def _():
            ptid().start()

    def arrive2(j):
        @pl.when(has_down2)
        def _():
            h2(j).wait_recv()

            @pl.when(odd == 1)
            def _():
                pt(j).start()

    arrive2(0)

    @pl.when(b >= 1)
    def _():
        ptid().wait_recv()
        make_bias(1)

    for copy in own_q:
        copy.wait()
    for k, _, frm in peers:
        st_in(k, frm, frm, at(b, frm)).wait_recv()

    tile = min(TILE, R)
    steps = R // tile
    per = tile // T if tile >= T else 1

    def stat_row(row, qt):
        parts = [statb[qt * per + i, pl.ds(row, 1), :] for i in range(per)]
        return parts[0] if per == 1 else jnp.concatenate(parts, axis=1)

    def hop_grads(hop, j, acc):
        def key_step(kt, _):
            krow = pl.ds(pl.multiple_of(kt * tile, tile), tile)
            kc = kvb[hop, 0, krow, cols(j * D, D)]
            vc = kvb[hop, 1, krow, cols(j * D, D)]

            def query_step(qt, carry):
                dk, dv = carry
                qrow = pl.ds(pl.multiple_of(qt * tile, tile), tile)
                for g in range(GROUP):
                    qc = qb[qrow, cols(j * GD + g * D, D)]
                    dc = dob[qrow, cols(j * GD + g * D, D)]
                    head = j * GROUP + g
                    lse = stat_row(head, qt)
                    delta = stat_row(G + head, qt)
                    w = jnp.exp(dot_nt(kc, qc) * scale - lse + bias[hop, krow, pl.ds(pl.multiple_of(qt * tile, tile), tile)])
                    dv = dv + dot_nn(w.astype(jnp.bfloat16), dc)
                    ds = (w * (dot_nt(vc, dc) - delta)).astype(jnp.bfloat16)
                    dk = dk + dot_nn(ds, qc)
                    part = dot_tn(ds, kc)
                    dqacc[qrow, g * D:(g + 1) * D] += part
                return dk, dv

            zero = jnp.zeros((tile, D), jnp.float32)
            if steps == 1:
                dk, dv = query_step(0, (zero, zero))
            else:
                dk, dv = lax.fori_loop(0, steps, query_step, (zero, zero))
            acc[j, 0, krow, :] = (dk * scale).astype(acc.dtype)
            acc[j, 1, krow, :] = dv.astype(acc.dtype)
            return 0

        if steps == 1:
            key_step(0, 0)
        else:
            lax.fori_loop(0, steps, key_step, 0)

    def give1(j):
        return rcopy(ret1.at[j], in1.at[j], r1_s.at[j], r1_r.at[j], at(mate, u))

    def give2(j):
        return rcopy(ret2.at[j], in2.at[j], r2_s.at[j], r2_r.at[j], at(b - 2, u))

    def oq(k, j, place, dev):
        return rcopy(
            dqs.at[j, rows(place), :], dq_ref.at[:, cols((u * KH + j) * GD, GD)],
            oq_s.at[j, k - 1], oq_r.at[j, k - 1], dev,
        )

    def okv(k, which, j, place, dev):
        ref = (dk_ref, dv_ref)[which]
        return rcopy(
            dkvs.at[j, which, rows(place), :], ref.at[:, cols((u * KH + j) * D, D)],
            okv_s.at[which, j, k - 1], okv_r.at[which, j, k - 1], dev,
        )

    def keep_q(j):
        return pltpu.make_async_copy(
            dqs.at[j, rows(u), :], dq_ref.at[:, cols((u * KH + j) * GD, GD)], keep_sem.at[2, j]
        )

    def keep_kv(which, j):
        ref = (dk_ref, dv_ref)[which]
        return pltpu.make_async_copy(
            dkvs.at[j, which, rows(u), :], ref.at[:, cols((u * KH + j) * D, D)],
            keep_sem.at[which, j],
        )

    def compute(j):
        for k, _, frm in peers:
            for which in range(2):
                qd_in(k, which, j, frm, frm, at(b, frm)).wait_recv()
        dqacc[...] = jnp.zeros_like(dqacc)

        @pl.when(b >= 1)
        def _():
            pt(j).wait_recv()
            hop_grads(1, j, ret1)
            give1(j).start()

        @pl.when(has_down2)
        def _():
            hop_grads(2, j, acc2)

        stage_a(j)
        hop_grads(0, j, acc0)

        dqs[j] = (dqacc[...] * scale).astype(jnp.bfloat16)
        for k, to, _ in peers:
            oq(k, j, to, at(b, to)).start()
        keep_q(j).start()

    def stage_a(j):
        @pl.when(jnp.logical_and(odd == 1, has_down2))
        def _():
            give1(j).wait_recv()
            ret2[j] = (acc2[j] + in1[j].astype(jnp.float32)).astype(jnp.bfloat16)

        @pl.when(jnp.logical_and(even, has_down2))
        def _():
            ret2[j] = acc2[j].astype(jnp.bfloat16)

        @pl.when(has_down2)
        def _():
            give2(j).start()

    def stage_b(j):
        @pl.when(even)
        def _():
            give1(j).wait_recv()
            acc0[j] += in1[j].astype(jnp.float32)

        @pl.when(has_up2)
        def _():
            give2(j).wait_recv()
            acc0[j] += in2[j].astype(jnp.float32)

        dkvs[j] = acc0[j].astype(jnp.bfloat16)
        for k, to, _ in peers:
            for which in range(2):
                okv(k, which, j, to, at(b, to)).start()
        for which in range(2):
            keep_kv(which, j).start()

    def head_step(j, _):
        @pl.when(j + 1 < KH)
        def _():
            arrive2(jnp.minimum(j + 1, KH - 1))

        compute(j)

        @pl.when(j >= 2)
        def _():
            stage_b(jnp.maximum(j - 2, 0))

        return 0

    lax.fori_loop(0, KH, head_step, 0)
    if KH >= 2:
        stage_b(KH - 2)
    stage_b(KH - 1)

    for k, to, frm in peers:
        id_in(k, u, at(b, to)).wait_send()
        st_in(k, u, to, at(b, to)).wait_send()

    @pl.when(has_up2)
    def _():
        h2id().wait_send()

    @pl.when(sends_mate)
    def _():
        ptid().wait_send()

    def finish(j, _):
        keep_q(j).wait()
        for which in range(2):
            keep_kv(which, j).wait()
        for k, to, frm in peers:
            for which in range(2):
                kv_in(k, which, j, u, to, at(b, to)).wait_send()
                qd_in(k, which, j, u, to, at(b, to)).wait_send()

        @pl.when(has_up2)
        def _():
            h2(j).wait_send()

        @pl.when(sends_mate)
        def _():
            pt(j).wait_send()

        @pl.when(b >= 1)
        def _():
            give1(j).wait_send()

        @pl.when(has_down2)
        def _():
            give2(j).wait_send()

        for k, to, frm in peers:
            oq(k, j, to, at(b, to)).wait_send()
            for which in range(2):
                okv(k, which, j, to, at(b, to)).wait_send()
            rcopy(
                dqs.at[j, rows(frm), :], dq_ref.at[:, cols((frm * KH + j) * GD, GD)],
                oq_s.at[j, k - 1], oq_r.at[j, k - 1], at(b, frm),
            ).wait_recv()
            for which in range(2):
                ref = (dk_ref, dv_ref)[which]
                rcopy(
                    dkvs.at[j, which, rows(frm), :], ref.at[:, cols((frm * KH + j) * D, D)],
                    okv_s.at[which, j, k - 1], okv_r.at[which, j, k - 1], at(b, frm),
                ).wait_recv()
        return 0

    lax.fori_loop(0, KH, finish, 0)


def close_kernel(a_in, b_in, c_in, a_out, b_out, c_out, a_mid, b_mid, c_mid, in_sem, out_sem):
    moves = []
    for i, (src, mid, dst) in enumerate(
        [(a_in, a_mid, a_out), (b_in, b_mid, b_out), (c_in, c_mid, c_out)]
    ):
        height = src.shape[0] // PIECES
        for n in range(PIECES):
            part = pl.ds(n * height, height)
            moves.append((
                pltpu.make_async_copy(src.at[part], mid.at[part], in_sem.at[i, n]),
                pltpu.make_async_copy(mid.at[part], dst.at[part], out_sem.at[i, n]),
            ))
    for load, _ in moves:
        load.start()
    for load, store in moves:
        load.wait()
        store.start()
    for _, store in moves:
        store.wait()


def per_device(uly_count, blk_count, q, k, v, out, grad, lse_parts, segment_ids):
    U, B = uly_count, blk_count
    T = q.shape[0]
    R = T * U
    KH = KEY_VALUE_HEADS // U
    G = KH * GROUP
    D = HEAD_SIZE
    stat_rows = -(-2 * G // 8) * 8
    parts = lse_parts.transpose(1, 2, 0)
    ids = segment_ids.reshape(1, T)
    bf, f32 = jnp.bfloat16, jnp.float32
    n = max(U - 1, 1)
    dma = pltpu.SemaphoreType.DMA
    sems = []
    for shape in [(2, KH, n), (2, KH, n), (n,), (n,), (KH,), (1,), (KH,), (1,), (KH,), (KH,), (KH, n), (2, KH, n)]:
        sems += [dma(shape), dma(shape)]
    vm = pltpu.VMEM
    results = pl.pallas_call(
        functools.partial(kernel, U, B),
        out_shape=(
            jax.ShapeDtypeStruct(q.shape, bf),
            jax.ShapeDtypeStruct(k.shape, bf),
            jax.ShapeDtypeStruct(v.shape, bf),
        ),
        in_specs=[pl.BlockSpec(memory_space=pltpu.HBM)] * 7,
        out_specs=tuple([pl.BlockSpec(memory_space=pltpu.HBM)] * 3),
        scratch_shapes=[
            vm((R, G * D), bf),
            vm((R, G * D), bf),
            vm((3, 2, R, KH * D), bf),
            vm((U, stat_rows, T), f32),
            vm((3, U, 1, T), jnp.int32),
            vm((3, R, R), f32),
            vm((R, GROUP * D), f32),
            vm((KH, 2, R, D), f32),
            vm((KH, 2, R, D), f32),
            vm((KH, R, GROUP * D), bf),
            vm((KH, 2, R, D), bf),
            vm((KH, 2, R, D), bf),
            vm((KH, 2, R, D), bf),
            vm((KH, 2, R, D), bf),
            vm((KH, 2, R, D), bf),
            vm(q.shape, bf),
            vm(k.shape, bf),
            vm(v.shape, bf),
            vm(q.shape, bf),
            vm(parts.shape, f32),
            vm((1, T), jnp.int32),
            vm((U, stat_rows, T), f32),
            dma((11,)),
            dma((3, KH)),
        ] + sems,
        compiler_params=pltpu.CompilerParams(
            collective_id=0, has_side_effects=True, vmem_limit_bytes=56 << 20
        ),
    )(q, grad, k, v, out, parts, ids)
    hbm = [pl.BlockSpec(memory_space=pltpu.HBM)] * 3
    return pl.pallas_call(
        close_kernel,
        out_shape=tuple(jax.ShapeDtypeStruct(r.shape, r.dtype) for r in results),
        in_specs=hbm,
        out_specs=tuple(hbm),
        scratch_shapes=[vm(r.shape, r.dtype) for r in results]
        + [dma((3, PIECES)), dma((3, PIECES))],
        compiler_params=pltpu.CompilerParams(vmem_limit_bytes=56 << 20),
    )(*results)


def solution(mesh):
    spec = P(("blk", "uly"), None)
    body = functools.partial(per_device, mesh.shape["uly"], mesh.shape["blk"])
    return jax.shard_map(
        body,
        mesh=mesh,
        in_specs=(spec, spec, spec, spec, spec, P(("blk", "uly"), None, None), P(("blk", "uly"))),
        out_specs=(spec, spec, spec),
        check_vma=False,
    )
```

```python
import functools
import math

import jax
import jax.numpy as jnp
from jax import lax
from jax.experimental import pallas as pl
from jax.experimental.pallas import tpu as pltpu
from jax.sharding import PartitionSpec as P

HEAD_SIZE = 128
QUERY_HEADS = 16
KEY_VALUE_HEADS = 8
GROUP = QUERY_HEADS // KEY_VALUE_HEADS
TILE = 256
PIECES = 2
FAR = -1e30


def dot_nt(a, b):
    return lax.dot_general(a, b, (((1,), (1,)), ((), ())), preferred_element_type=jnp.float32)


def dot_nn(a, b):
    return lax.dot_general(a, b, (((1,), (0,)), ((), ())), preferred_element_type=jnp.float32)


def dot_tn(a, b):
    return lax.dot_general(a, b, (((0,), (0,)), ((), ())), preferred_element_type=jnp.float32)


def kernel(
    uly_count, blk_count,
    q_ref, do_hbm, k_hbm, v_hbm, out_hbm, lp_hbm, ids_hbm,
    dq_ref, dk_ref, dv_ref,
    qb, dob, kvb, statb, idb, bias,
    dqacc, acc0, acc2, dqs, ret1, ret2, in1, in2, dkvs,
    do_ref, k_ref, v_ref, out_ref, lp_ref, ids_ref, stat_ref,
    loc_sem, keep_sem,
    kv_s, kv_r, qd_s, qd_r, st_s, st_r, id_s, id_r,
    h2_s, h2_r, h2i_s, h2i_r, pt_s, pt_r, pti_s, pti_r,
    r1_s, r1_r, r2_s, r2_r, oq_s, oq_r, okv_s, okv_r,
):
    U, B = uly_count, blk_count
    T = q_ref.shape[0]
    R = T * U
    KH = KEY_VALUE_HEADS // U
    D = HEAD_SIZE
    GD = GROUP * D
    scale = 1.0 / math.sqrt(D)
    u = lax.axis_index("uly")
    b = lax.axis_index("blk")
    odd = lax.rem(b, 2)
    even = odd == 0
    mate = b + 1 - 2 * odd

    def at(blk, uly):
        return {"blk": blk, "uly": uly}

    def rcopy(src, dst, ssem, rsem, dev):
        return pltpu.make_async_remote_copy(
            src_ref=src, dst_ref=dst, send_sem=ssem, recv_sem=rsem,
            device_id=dev, device_id_type=pl.DeviceIdType.MESH,
        )

    def cols(first, width):
        return pl.ds(pl.multiple_of(first, 128), width)

    def rows(place):
        return pl.ds(pl.multiple_of(place * T, T), T)

    has_up2 = b + 2 < B
    has_down2 = b >= 2
    sends_mate = jnp.logical_or(even, b >= 3)

    loads = [
        pltpu.make_async_copy(src, dst, loc_sem.at[5 + i])
        for i, (src, dst) in enumerate([
            (ids_hbm, ids_ref), (k_hbm, k_ref), (v_hbm, v_ref),
            (do_hbm, do_ref), (out_hbm, out_ref), (lp_hbm, lp_ref),
        ])
    ]
    own_kv = [
        pltpu.make_async_copy(
            k_hbm.at[:, cols(u * KH * D, KH * D)], kvb.at[0, 0, rows(u), :], loc_sem.at[2]
        ),
        pltpu.make_async_copy(
            v_hbm.at[:, cols(u * KH * D, KH * D)], kvb.at[0, 1, rows(u), :], loc_sem.at[3]
        ),
    ]
    for copy in own_kv + loads:
        copy.start()

    barrier = pltpu.get_barrier_semaphore()
    for k in range(1, U):
        pl.semaphore_signal(
            barrier, inc=1, device_id=at(b, lax.rem(u + k, U)), device_id_type=pl.DeviceIdType.MESH
        )
    pl.semaphore_signal(barrier, inc=1, device_id=at(mate, u), device_id_type=pl.DeviceIdType.MESH)

    @pl.when(has_up2)
    def _():
        pl.semaphore_signal(
            barrier, inc=1, device_id=at(b + 2, u), device_id_type=pl.DeviceIdType.MESH
        )

    @pl.when(has_down2)
    def _():
        pl.semaphore_signal(
            barrier, inc=1, device_id=at(b - 2, u), device_id_type=pl.DeviceIdType.MESH
        )

    expected = U + has_up2.astype(jnp.int32) + has_down2.astype(jnp.int32)
    pl.semaphore_wait(barrier, expected)

    own_q = [
        pltpu.make_async_copy(
            q_ref.at[:, cols(u * KH * GD, KH * GD)], qb.at[rows(u), :], loc_sem.at[0]
        ),
        pltpu.make_async_copy(
            do_hbm.at[:, cols(u * KH * GD, KH * GD)], dob.at[rows(u), :], loc_sem.at[1]
        ),
    ]
    own_id = pltpu.make_async_copy(ids_hbm, idb.at[0, u], loc_sem.at[4])

    def id_in(k, place, dev):
        return rcopy(ids_ref, idb.at[0, place], id_s.at[k - 1], id_r.at[k - 1], dev)

    def st_in(k, place, peer, dev):
        return rcopy(stat_ref.at[peer], statb.at[place], st_s.at[k - 1], st_r.at[k - 1], dev)

    def kv_in(k, which, j, place, peer, dev):
        ref = (k_ref, v_ref)[which]
        return rcopy(
            ref.at[:, cols((peer * KH + j) * D, D)],
            kvb.at[0, which, rows(place), cols(j * D, D)],
            kv_s.at[which, j, k - 1], kv_r.at[which, j, k - 1], dev,
        )

    def qd_in(k, which, j, place, peer, dev):
        ref, buf = ((q_ref, qb), (do_ref, dob))[which]
        return rcopy(
            ref.at[:, cols((peer * KH + j) * GD, GD)],
            buf.at[rows(place), cols(j * GD, GD)],
            qd_s.at[which, j, k - 1], qd_r.at[which, j, k - 1], dev,
        )

    def h2(j, i, place):
        return rcopy(
            kvb.at[0, :, rows(place), cols(j * D, D)], kvb.at[2, :, rows(place), cols(j * D, D)],
            h2_s.at[j, i], h2_r.at[j, i], at(b + 2, u),
        )

    peers = [(k, lax.rem(u + k, U), lax.rem(u + U - k, U)) for k in range(1, U)]
    shares = [(0, u)] + [(k, frm) for k, _, frm in peers]
    for copy in own_kv:
        copy.wait()

    @pl.when(has_up2)
    def _():
        for j in range(KH):
            h2(j, 0, u).start()

    loads[0].wait()
    for k, to, _ in peers:
        id_in(k, u, at(b, to)).start()
    loads[1].wait()
    loads[2].wait()
    for j in range(KH):
        for k, to, _ in peers:
            for which in range(2):
                kv_in(k, which, j, u, to, at(b, to)).start()
    for copy in [own_id] + own_q:
        copy.start()

    for copy in loads[3:]:
        copy.wait()
    G = KH * GROUP
    lane = lax.broadcasted_iota(jnp.int32, (T, 128), 1)
    table = jnp.zeros((T, 128), jnp.float32)
    for h in range(U * G):
        piece = slice(h * D, (h + 1) * D)
        total = jnp.sum(
            do_ref[:, piece].astype(jnp.float32) * out_ref[:, piece].astype(jnp.float32),
            axis=1, keepdims=True,
        )
        table = jnp.where(lane == h, total, table)
    table = table.T
    part0, part1 = lp_ref[:, 0, :], lp_ref[:, 1, :]
    highest = jnp.maximum(part0, part1)
    lse_rows = highest + jnp.log(jnp.exp(part0 - highest) + jnp.exp(part1 - highest))
    for p in range(U):
        stat_ref[p, :G, :] = lse_rows[p * G:(p + 1) * G]
        stat_ref[p, G:2 * G, :] = table[p * G:(p + 1) * G]
    statb[u] = stat_ref[u]

    for j in range(KH):
        for k, to, _ in peers:
            for which in range(2):
                qd_in(k, which, j, u, to, at(b, to)).start()
        if j == 0:
            for k, to, _ in peers:
                st_in(k, u, to, at(b, to)).start()


    def h2id():
        return rcopy(idb.at[0], idb.at[2], h2i_s.at[0], h2i_r.at[0], at(b + 2, u))

    def pt(j):
        return rcopy(
            kvb.at[2 * odd, :, :, cols(j * D, D)], kvb.at[1, :, :, cols(j * D, D)],
            pt_s.at[j], pt_r.at[j], at(mate, u),
        )

    def ptid():
        return rcopy(idb.at[2 * odd], idb.at[1], pti_s.at[0], pti_r.at[0], at(mate, u))

    own_id.wait()
    for k, _, frm in peers:
        id_in(k, frm, at(b, frm)).wait_recv()

    @pl.when(has_up2)
    def _():
        h2id().start()

    @pl.when(even)
    def _():
        ptid().start()

    for j in range(KH):
        for k, _, frm in peers:
            for which in range(2):
                kv_in(k, which, j, frm, frm, at(b, frm)).wait_recv()

        @pl.when(has_up2)
        def _():
            for k, _, frm in peers:
                h2(j, k, frm).start()

        @pl.when(even)
        def _():
            pt(j).start()

    def make_bias(hop):
        for kp in range(U):
            key_ids = jnp.broadcast_to(idb[hop, kp, 0:1, :].astype(jnp.float32), (T, T)).T
            for qp in range(U):
                query_ids = idb[0, qp, 0:1, :].astype(jnp.float32)
                good = key_ids == query_ids
                if hop == 0:
                    kpos = lax.broadcasted_iota(jnp.int32, (T, T), 0) + kp * T
                    qpos = lax.broadcasted_iota(jnp.int32, (T, T), 1) + qp * T
                    good = jnp.logical_and(good, kpos <= qpos)
                bias[hop, kp * T:(kp + 1) * T, qp * T:(qp + 1) * T] = jnp.where(good, 0.0, FAR)

    make_bias(0)

    @pl.when(has_down2)
    def _():
        h2id().wait_recv()
        make_bias(2)

        @pl.when(odd == 1)
        def _():
            ptid().start()

    def arrive2(j):
        @pl.when(has_down2)
        def _():
            for i, place in shares:
                h2(j, i, place).wait_recv()

            @pl.when(odd == 1)
            def _():
                pt(j).start()

    arrive2(0)

    @pl.when(b >= 1)
    def _():
        ptid().wait_recv()
        make_bias(1)

    for copy in own_q:
        copy.wait()
    for k, _, frm in peers:
        st_in(k, frm, frm, at(b, frm)).wait_recv()

    tile = min(TILE, R)
    steps = R // tile
    per = tile // T if tile >= T else 1

    def stat_row(row, qt):
        parts = [statb[qt * per + i, pl.ds(row, 1), :] for i in range(per)]
        return parts[0] if per == 1 else jnp.concatenate(parts, axis=1)

    def hop_grads(hop, j, acc):
        def key_step(kt, _):
            krow = pl.ds(pl.multiple_of(kt * tile, tile), tile)
            kc = kvb[hop, 0, krow, cols(j * D, D)]
            vc = kvb[hop, 1, krow, cols(j * D, D)]

            def query_step(qt, carry):
                dk, dv = carry
                qrow = pl.ds(pl.multiple_of(qt * tile, tile), tile)
                for g in range(GROUP):
                    qc = qb[qrow, cols(j * GD + g * D, D)]
                    dc = dob[qrow, cols(j * GD + g * D, D)]
                    head = j * GROUP + g
                    lse = stat_row(head, qt)
                    delta = stat_row(G + head, qt)
                    w = jnp.exp(dot_nt(kc, qc) * scale - lse + bias[hop, krow, pl.ds(pl.multiple_of(qt * tile, tile), tile)])
                    dv = dv + dot_nn(w.astype(jnp.bfloat16), dc)
                    ds = (w * (dot_nt(vc, dc) - delta)).astype(jnp.bfloat16)
                    dk = dk + dot_nn(ds, qc)
                    part = dot_tn(ds, kc)
                    dqacc[qrow, g * D:(g + 1) * D] += part
                return dk, dv

            zero = jnp.zeros((tile, D), jnp.float32)
            if steps == 1:
                dk, dv = query_step(0, (zero, zero))
            else:
                dk, dv = lax.fori_loop(0, steps, query_step, (zero, zero))
            acc[j, 0, krow, :] = (dk * scale).astype(acc.dtype)
            acc[j, 1, krow, :] = dv.astype(acc.dtype)
            return 0

        if steps == 1:
            key_step(0, 0)
        else:
            lax.fori_loop(0, steps, key_step, 0)

    def give1(j):
        return rcopy(ret1.at[j], in1.at[j], r1_s.at[j], r1_r.at[j], at(mate, u))

    def give2(j):
        return rcopy(ret2.at[j], in2.at[j], r2_s.at[j], r2_r.at[j], at(b - 2, u))

    def oq(k, j, place, dev):
        return rcopy(
            dqs.at[j, rows(place), :], dq_ref.at[:, cols((u * KH + j) * GD, GD)],
            oq_s.at[j, k - 1], oq_r.at[j, k - 1], dev,
        )

    def okv(k, which, j, place, dev):
        ref = (dk_ref, dv_ref)[which]
        return rcopy(
            dkvs.at[j, which, rows(place), :], ref.at[:, cols((u * KH + j) * D, D)],
            okv_s.at[which, j, k - 1], okv_r.at[which, j, k - 1], dev,
        )

    def keep_q(j):
        return pltpu.make_async_copy(
            dqs.at[j, rows(u), :], dq_ref.at[:, cols((u * KH + j) * GD, GD)], keep_sem.at[2, j]
        )

    def keep_kv(which, j):
        ref = (dk_ref, dv_ref)[which]
        return pltpu.make_async_copy(
            dkvs.at[j, which, rows(u), :], ref.at[:, cols((u * KH + j) * D, D)],
            keep_sem.at[which, j],
        )

    def compute(j):
        for k, _, frm in peers:
            for which in range(2):
                qd_in(k, which, j, frm, frm, at(b, frm)).wait_recv()
        dqacc[...] = jnp.zeros_like(dqacc)

        @pl.when(b >= 1)
        def _():
            pt(j).wait_recv()
            hop_grads(1, j, ret1)
            give1(j).start()

        @pl.when(has_down2)
        def _():
            hop_grads(2, j, acc2)

        stage_a(j)
        hop_grads(0, j, acc0)

        dqs[j] = (dqacc[...] * scale).astype(jnp.bfloat16)
        for k, to, _ in peers:
            oq(k, j, to, at(b, to)).start()
        keep_q(j).start()

    def stage_a(j):
        @pl.when(jnp.logical_and(odd == 1, has_down2))
        def _():
            give1(j).wait_recv()
            ret2[j] = (acc2[j] + in1[j].astype(jnp.float32)).astype(jnp.bfloat16)

        @pl.when(jnp.logical_and(even, has_down2))
        def _():
            ret2[j] = acc2[j].astype(jnp.bfloat16)

        @pl.when(has_down2)
        def _():
            give2(j).start()

    def stage_b(j):
        @pl.when(even)
        def _():
            give1(j).wait_recv()
            acc0[j] += in1[j].astype(jnp.float32)

        @pl.when(has_up2)
        def _():
            give2(j).wait_recv()
            acc0[j] += in2[j].astype(jnp.float32)

        dkvs[j] = acc0[j].astype(jnp.bfloat16)
        for k, to, _ in peers:
            for which in range(2):
                okv(k, which, j, to, at(b, to)).start()
        for which in range(2):
            keep_kv(which, j).start()

    def head_step(j, _):
        @pl.when(j + 1 < KH)
        def _():
            arrive2(jnp.minimum(j + 1, KH - 1))

        compute(j)

        @pl.when(j >= 2)
        def _():
            stage_b(jnp.maximum(j - 2, 0))

        return 0

    lax.fori_loop(0, KH, head_step, 0)
    if KH >= 2:
        stage_b(KH - 2)
    stage_b(KH - 1)

    for k, to, frm in peers:
        id_in(k, u, at(b, to)).wait_send()
        st_in(k, u, to, at(b, to)).wait_send()

    @pl.when(has_up2)
    def _():
        h2id().wait_send()

    @pl.when(sends_mate)
    def _():
        ptid().wait_send()

    def finish(j, _):
        keep_q(j).wait()
        for which in range(2):
            keep_kv(which, j).wait()
        for k, to, frm in peers:
            for which in range(2):
                kv_in(k, which, j, u, to, at(b, to)).wait_send()
                qd_in(k, which, j, u, to, at(b, to)).wait_send()

        @pl.when(has_up2)
        def _():
            for i, place in shares:
                h2(j, i, place).wait_send()

        @pl.when(sends_mate)
        def _():
            pt(j).wait_send()

        @pl.when(b >= 1)
        def _():
            give1(j).wait_send()

        @pl.when(has_down2)
        def _():
            give2(j).wait_send()

        for k, to, frm in peers:
            oq(k, j, to, at(b, to)).wait_send()
            for which in range(2):
                okv(k, which, j, to, at(b, to)).wait_send()
            rcopy(
                dqs.at[j, rows(frm), :], dq_ref.at[:, cols((frm * KH + j) * GD, GD)],
                oq_s.at[j, k - 1], oq_r.at[j, k - 1], at(b, frm),
            ).wait_recv()
            for which in range(2):
                ref = (dk_ref, dv_ref)[which]
                rcopy(
                    dkvs.at[j, which, rows(frm), :], ref.at[:, cols((frm * KH + j) * D, D)],
                    okv_s.at[which, j, k - 1], okv_r.at[which, j, k - 1], at(b, frm),
                ).wait_recv()
        return 0

    lax.fori_loop(0, KH, finish, 0)


def close_kernel(a_in, b_in, c_in, a_out, b_out, c_out, a_mid, b_mid, c_mid, in_sem, out_sem):
    moves = []
    for i, (src, mid, dst) in enumerate(
        [(a_in, a_mid, a_out), (b_in, b_mid, b_out), (c_in, c_mid, c_out)]
    ):
        height = src.shape[0] // PIECES
        for n in range(PIECES):
            part = pl.ds(n * height, height)
            moves.append((
                pltpu.make_async_copy(src.at[part], mid.at[part], in_sem.at[i, n]),
                pltpu.make_async_copy(mid.at[part], dst.at[part], out_sem.at[i, n]),
            ))
    for load, _ in moves:
        load.start()
    for load, store in moves:
        load.wait()
        store.start()
    for _, store in moves:
        store.wait()


def per_device(uly_count, blk_count, q, k, v, out, grad, lse_parts, segment_ids):
    U, B = uly_count, blk_count
    T = q.shape[0]
    R = T * U
    KH = KEY_VALUE_HEADS // U
    G = KH * GROUP
    D = HEAD_SIZE
    stat_rows = -(-2 * G // 8) * 8
    parts = lse_parts.transpose(1, 2, 0)
    ids = segment_ids.reshape(1, T)
    bf, f32 = jnp.bfloat16, jnp.float32
    n = max(U - 1, 1)
    dma = pltpu.SemaphoreType.DMA
    sems = []
    for shape in [(2, KH, n), (2, KH, n), (n,), (n,), (KH, U), (1,), (KH,), (1,), (KH,), (KH,), (KH, n), (2, KH, n)]:
        sems += [dma(shape), dma(shape)]
    vm = pltpu.VMEM
    results = pl.pallas_call(
        functools.partial(kernel, U, B),
        out_shape=(
            jax.ShapeDtypeStruct(q.shape, bf),
            jax.ShapeDtypeStruct(k.shape, bf),
            jax.ShapeDtypeStruct(v.shape, bf),
        ),
        in_specs=[pl.BlockSpec(memory_space=pltpu.HBM)] * 7,
        out_specs=tuple([pl.BlockSpec(memory_space=pltpu.HBM)] * 3),
        scratch_shapes=[
            vm((R, G * D), bf),
            vm((R, G * D), bf),
            vm((3, 2, R, KH * D), bf),
            vm((U, stat_rows, T), f32),
            vm((3, U, 1, T), jnp.int32),
            vm((3, R, R), f32),
            vm((R, GROUP * D), f32),
            vm((KH, 2, R, D), f32),
            vm((KH, 2, R, D), f32),
            vm((KH, R, GROUP * D), bf),
            vm((KH, 2, R, D), bf),
            vm((KH, 2, R, D), bf),
            vm((KH, 2, R, D), bf),
            vm((KH, 2, R, D), bf),
            vm((KH, 2, R, D), bf),
            vm(q.shape, bf),
            vm(k.shape, bf),
            vm(v.shape, bf),
            vm(q.shape, bf),
            vm(parts.shape, f32),
            vm((1, T), jnp.int32),
            vm((U, stat_rows, T), f32),
            dma((11,)),
            dma((3, KH)),
        ] + sems,
        compiler_params=pltpu.CompilerParams(
            collective_id=0, has_side_effects=True, vmem_limit_bytes=56 << 20
        ),
    )(q, grad, k, v, out, parts, ids)
    hbm = [pl.BlockSpec(memory_space=pltpu.HBM)] * 3
    return pl.pallas_call(
        close_kernel,
        out_shape=tuple(jax.ShapeDtypeStruct(r.shape, r.dtype) for r in results),
        in_specs=hbm,
        out_specs=tuple(hbm),
        scratch_shapes=[vm(r.shape, r.dtype) for r in results]
        + [dma((3, PIECES)), dma((3, PIECES))],
        compiler_params=pltpu.CompilerParams(vmem_limit_bytes=56 << 20),
    )(*results)


def solution(mesh):
    spec = P(("blk", "uly"), None)
    body = functools.partial(per_device, mesh.shape["uly"], mesh.shape["blk"])
    return jax.shard_map(
        body,
        mesh=mesh,
        in_specs=(spec, spec, spec, spec, spec, P(("blk", "uly"), None, None), P(("blk", "uly"))),
        out_specs=(spec, spec, spec),
        check_vma=False,
    )
```
